8 devices in a mesh: dp: 1 (over z), beam: 8 (over y, x, core).
Axes of the slice: x: 2, y: 2, z: 1, core: 2. Of those that a mesh axis runs over, the one named last changes fastest.
Arguments:
- emb_one: bfloat16 [64, 4096], P(('dp', 'beam'))
- emb_two: bfloat16 [64, 4096], P(('dp', 'beam'))
- parent_one: int32 [1, 64], P('dp')
- parent_two: int32 [1, 64], P('dp')
- position: int32 [], replicated
- scores: float32 [64], P(('dp', 'beam'))
- k_cache0: bfloat16 [64, 128, 8, 128], P(('dp', 'beam'))
- v_cache0: bfloat16 [64, 128, 8, 128], P(('dp', 'beam'))
- k_cache1: bfloat16 [64, 128, 8, 128], P(('dp', 'beam'))
- v_cache1: bfloat16 [64, 128, 8, 128], P(('dp', 'beam'))
- w_query: bfloat16 [2, 4096, 4096], replicated
- w_key: bfloat16 [2, 4096, 1024], replicated
- w_value: bfloat16 [2, 4096, 1024], replicated
- w_out: bfloat16 [2, 4096, 4096], replicated
- w_gate: bfloat16 [2, 4096, 14336], replicated
- w_up: bfloat16 [2, 4096, 14336], replicated
- w_down: bfloat16 [2, 14336, 4096], replicated
- g_attn: float32 [2, 4096], replicated
- g_mlp: float32 [2, 4096], replicated
- g_final: float32 [4096], replicated
- w_vocab: bfloat16 [4096, 32000], replicated
Outputs:
- output 1: bfloat16 [64, 128, 8, 128], P(('dp', 'beam'))
- output 2: bfloat16 [64, 128, 8, 128], P(('dp', 'beam'))
- output 3: bfloat16 [64, 128, 8, 128], P(('dp', 'beam'))
- output 4: bfloat16 [64, 128, 8, 128], P(('dp', 'beam'))
- output 5: float32 [64, 32000], P(('dp', 'beam'))
- output 6: float32 [64, 32000], P(('dp', 'beam'))
All inputs are finite; a program needn't handle non-finite values.
Results may differ from the reference program's by a relative error of at most 0.00101094.
Values are sent between devices in bfloat16 or wider.
A program may use at most 4.5 GiB of HBM per device.

```python
import jax
import jax.numpy as jnp
from jax import lax

BEAMS = 64
BEAM_WIDTH = 64
SEQ = 128
D_MODEL = 4096
HEADS = 32
KV_HEADS = 8
HEAD = 128
FF = 14336
VOCAB = 32000
LAYERS = 2
SENTENCES = BEAMS // BEAM_WIDTH
EPS = 1e-6
ROPE_BASE = 1.0e4


def draw_parent(rand_key):
    key_dom, key_flip, key_any = jax.random.split(rand_key, 3)
    dominant = jax.random.randint(key_dom, (SENTENCES, 1), 0, BEAM_WIDTH, dtype=jnp.int32)
    coin_flip = jax.random.randint(key_flip, (SENTENCES, BEAM_WIDTH), 0, 2, dtype=jnp.int32)
    anywhere = jax.random.randint(key_any, (SENTENCES, BEAM_WIDTH), 0, BEAM_WIDTH, dtype=jnp.int32)
    return jnp.where(coin_flip == 1, dominant, anywhere)


def draw_values(rand_key):
    key_centre, key_noise = jax.random.split(rand_key)
    centre = jax.random.normal(key_centre, (BEAMS, 1, KV_HEADS, HEAD), jnp.float32)
    noise_val = jax.random.normal(key_noise, (BEAMS, SEQ, KV_HEADS, HEAD), jnp.float32)
    return (centre + 0.5 * noise_val).astype(jnp.bfloat16)


def draw_weight(rand_key, shape_of, scale_val):
    return (jax.random.normal(rand_key, shape_of, jnp.float32) * scale_val).astype(jnp.bfloat16)


def setup_inputs(seed: int = 0, part: int = 0) -> dict:
    part_keys = jax.random.split(jax.random.fold_in(jax.random.key(seed), part), 9)
    shared_keys = jax.random.split(jax.random.key(seed + 1), 12)
    width_q = HEADS * HEAD
    width_kv = KV_HEADS * HEAD
    cache_shape = (BEAMS, SEQ, KV_HEADS, HEAD)
    scale_model = D_MODEL ** -0.5
    scale_query = width_q ** -0.5
    scale_hidden = FF ** -0.5
    scale_vocab = 2.0 * scale_model
    return {
        'emb_one': jax.random.normal(part_keys[0], (BEAMS, D_MODEL), jnp.float32).astype(jnp.bfloat16),
        'emb_two': jax.random.normal(part_keys[1], (BEAMS, D_MODEL), jnp.float32).astype(jnp.bfloat16),
        'parent_one': draw_parent(part_keys[2]),
        'parent_two': draw_parent(part_keys[3]),
        'position': jax.random.randint(shared_keys[0], (), SEQ // 2, SEQ - 1, dtype=jnp.int32),
        'scores': -1.0 - 4.0 * jax.random.uniform(part_keys[4], (BEAMS,), jnp.float32),
        'k_cache0': jax.random.normal(part_keys[5], cache_shape, jnp.float32).astype(jnp.bfloat16),
        'v_cache0': draw_values(part_keys[6]),
        'k_cache1': jax.random.normal(part_keys[7], cache_shape, jnp.float32).astype(jnp.bfloat16),
        'v_cache1': draw_values(part_keys[8]),
        'w_query': draw_weight(shared_keys[1], (LAYERS, D_MODEL, width_q), scale_model),
        'w_key': draw_weight(shared_keys[2], (LAYERS, D_MODEL, width_kv), scale_model),
        'w_value': draw_weight(shared_keys[3], (LAYERS, D_MODEL, width_kv), scale_model),
        'w_out': draw_weight(shared_keys[4], (LAYERS, width_q, D_MODEL), scale_query),
        'w_gate': draw_weight(shared_keys[5], (LAYERS, D_MODEL, FF), scale_model),
        'w_up': draw_weight(shared_keys[6], (LAYERS, D_MODEL, FF), scale_model),
        'w_down': draw_weight(shared_keys[7], (LAYERS, FF, D_MODEL), scale_hidden),
        'g_attn': 1.0 + 0.3 * jax.random.normal(shared_keys[8], (LAYERS, D_MODEL), jnp.float32),
        'g_mlp': 1.0 + 0.3 * jax.random.normal(shared_keys[9], (LAYERS, D_MODEL), jnp.float32),
        'g_final': 1.0 + 0.3 * jax.random.normal(shared_keys[10], (D_MODEL,), jnp.float32),
        'w_vocab': draw_weight(shared_keys[11], (D_MODEL, VOCAB), scale_vocab),
    }


def rms_norm(residual, gain_vec):
    mean_sq = jnp.mean(residual * residual, axis=-1, keepdims=True)
    return (residual * lax.rsqrt(mean_sq + EPS) * gain_vec).astype(jnp.bfloat16)


def rotate(vectors, position):
    half_dim = HEAD // 2
    inv_freq = ROPE_BASE ** (-2.0 * jnp.arange(half_dim, dtype=jnp.float32) / HEAD)
    angles = position.astype(jnp.float32) * inv_freq
    cosine = jnp.cos(angles)
    sine_val = jnp.sin(angles)
    lower_half = vectors[..., :half_dim]
    upper_half = vectors[..., half_dim:]
    return jnp.concatenate([lower_half * cosine - upper_half * sine_val, upper_half * cosine + lower_half * sine_val], axis=-1)


def attend(queries, k_rows, v_rows, position):
    grouped = queries.reshape(BEAMS, KV_HEADS, HEADS // KV_HEADS, HEAD).astype(jnp.float32)
    logits = jnp.einsum('bkgd,bskd->bkgs', grouped, k_rows.astype(jnp.float32)) * HEAD ** -0.5
    valid_slot = jnp.arange(SEQ) <= position
    logits = jnp.where(valid_slot, logits, -jnp.inf)
    attn_probs = jax.nn.softmax(logits, axis=-1).astype(jnp.bfloat16)
    attn_out = jnp.einsum('bkgs,bskd->bkgd', attn_probs.astype(jnp.float32), v_rows.astype(jnp.float32))
    return attn_out.astype(jnp.bfloat16).reshape(BEAMS, HEADS * HEAD)


def run_layer(residual, k_rows, v_rows, position, layer_idx, weights):
    w_query, w_key, w_value, w_out, w_gate, w_up, w_down, g_attn, g_mlp = weights
    normed = rms_norm(residual, g_attn[layer_idx])
    queries = jnp.dot(normed, w_query[layer_idx], preferred_element_type=jnp.float32).reshape(BEAMS, HEADS, HEAD)
    k_new = jnp.dot(normed, w_key[layer_idx], preferred_element_type=jnp.float32).reshape(BEAMS, KV_HEADS, HEAD)
    v_new = jnp.dot(normed, w_value[layer_idx], preferred_element_type=jnp.float32).reshape(BEAMS, KV_HEADS, HEAD)
    queries = rotate(queries, position).astype(jnp.bfloat16)
    k_new = rotate(k_new, position).astype(jnp.bfloat16)
    zero_idx = jnp.zeros_like(position)
    k_rows = lax.dynamic_update_slice(k_rows, k_new[:, None], (zero_idx, position, zero_idx, zero_idx))
    v_rows = lax.dynamic_update_slice(v_rows, v_new.astype(jnp.bfloat16)[:, None], (zero_idx, position, zero_idx, zero_idx))
    attn_out = attend(queries, k_rows, v_rows, position)
    residual = residual + jnp.dot(attn_out, w_out[layer_idx], preferred_element_type=jnp.float32)
    normed = rms_norm(residual, g_mlp[layer_idx])
    gate_val = jnp.dot(normed, w_gate[layer_idx], preferred_element_type=jnp.float32)
    up_val = jnp.dot(normed, w_up[layer_idx], preferred_element_type=jnp.float32)
    hidden = (jax.nn.silu(gate_val) * up_val).astype(jnp.bfloat16)
    residual = residual + jnp.dot(hidden, w_down[layer_idx], preferred_element_type=jnp.float32)
    return residual, k_rows, v_rows


def beam_sources(parents):
    return (jnp.arange(parents.shape[0], dtype=jnp.int32)[:, None] * parents.shape[1] + parents).reshape(-1)


def decode_step(embeds, sources, position, k_caches, v_caches, weights):
    residual = embeds.astype(jnp.float32)
    new_k = []
    new_v = []
    for layer_idx in range(LAYERS):
        k_rows = jnp.take(k_caches[layer_idx], sources, axis=0)
        v_rows = jnp.take(v_caches[layer_idx], sources, axis=0)
        residual, k_rows, v_rows = run_layer(residual, k_rows, v_rows, position, layer_idx, weights[:9])
        new_k.append(k_rows)
        new_v.append(v_rows)
    logits = jnp.dot(rms_norm(residual, weights[9]), weights[10], preferred_element_type=jnp.float32)
    return jax.nn.log_softmax(logits, axis=-1), new_k, new_v


def reference(emb_one, emb_two, parent_one, parent_two, position, scores, k_cache0, v_cache0, k_cache1, v_cache1, w_query, w_key, w_value, w_out, w_gate, w_up, w_down, g_attn, g_mlp, g_final, w_vocab):
    weights = (w_query, w_key, w_value, w_out, w_gate, w_up, w_down, g_attn, g_mlp, g_final, w_vocab)
    sources_one = beam_sources(parent_one)
    sources_two = beam_sources(parent_two)
    logp_one, k_mid, v_mid = decode_step(emb_one, sources_one, position, (k_cache0, k_cache1), (v_cache0, v_cache1), weights)
    logp_two, k_end, v_end = decode_step(emb_two, sources_two, position + 1, k_mid, v_mid, weights)
    score_one = jnp.take(scores, sources_one)
    score_two = jnp.take(score_one, sources_two)
    return (k_end[0], v_end[0], k_end[1], v_end[1], score_one[:, None] + logp_one, score_two[:, None] + logp_two)
```

```python
import functools

import jax
import jax.numpy as jnp
from jax import lax
from jax.experimental import pallas as pl
from jax.experimental.pallas import tpu as pltpu
from jax.sharding import PartitionSpec as P

EPS = 1e-6
ROPE_BASE = 1.0e4
CAP = 4
ALL = 16
ROWS = 32
SEQ = 128
HEAD = 128
KVH = 8
OWN = 8
GROUPS = 4
PEERS = 3
POS_A = 4 * HEAD
POS_B = 5 * HEAD
PAIR = 2 * HEAD
GB = 10 ** 9
BLK = 256
KCH = 512
LOW_VOCAB = 16128
MLP_SLOTS = 6
VOCAB_SLOTS = 16
VLIM = 58 * 1024 * 1024
F32 = jnp.float32
BF16 = jnp.bfloat16
VMEM = pl.BlockSpec(memory_space=pltpu.VMEM)
SMEM = pl.BlockSpec(memory_space=pltpu.SMEM)
HBM = pl.BlockSpec(memory_space=pl.ANY)
DMA = pltpu.SemaphoreType.DMA
MESH = pl.DeviceIdType.MESH
ROW = (SEQ, KVH, HEAD)


def shaped(shape, dtype):
    return jax.ShapeDtypeStruct(shape, dtype)


def dot(a, b):
    return jnp.dot(a, b, preferred_element_type=F32)


def call(kernel, name, flops, nbytes, ins, outs, out_shape, scratch, args, **extra):
    return pl.pallas_call(
        kernel, in_specs=ins, out_specs=outs, out_shape=out_shape, scratch_shapes=scratch, name=name,
        cost_estimate=pl.CostEstimate(flops=int(flops), bytes_accessed=int(nbytes), transcendentals=0),
        compiler_params=pltpu.CompilerParams(vmem_limit_bytes=VLIM, **extra))(*args)


def split(refs, *sizes):
    parts = []
    for n in sizes:
        parts.append(refs[:n])
        refs = refs[n:]
    return parts


def core_of():
    return lax.axis_index('beam') % 2


def xor_pairs(mask):
    return [(d, d ^ mask) for d in range(8)]


def swap(x, mask):
    return lax.ppermute(x, 'beam', xor_pairs(mask))


T_FROM = 3 * ALL
T_RANK = 4 * ALL
T_MOST = 5 * ALL
T_NEED = T_MOST + 1
T_END = T_NEED + ALL


def table_kernel(p1, p2, tab, rank, count):
    me = lax.axis_index('beam')
    core = me % 2
    chip = me // 2
    for i in range(BLK):
        rank[i] = -1
    for i in range(ALL):
        count[i] = 0
    for i in range(T_END):
        tab[i] = 0

    def beam(b, most):
        src = p1[0, p2[0, b]]
        row = src % ALL
        s = src // ALL
        d = b // ALL
        for needed in (p1[0, b], src):
            @pl.when(needed // ALL == chip)
            def _(needed=needed):
                tab[T_NEED + (needed % ALL ^ core * OWN)] = 1
        key = src * 4 + d
        pair = s * 4 + d
        fresh = rank[key] < 0
        here = jnp.where(fresh, count[pair], rank[key])
        rank[key] = here
        total = jnp.maximum(count[pair], here + 1)
        count[pair] = total

        @pl.when((s == chip) & (d != chip))
        def _():
            tab[((d ^ chip) - 1) * ALL + here] = row ^ (core * OWN)

        @pl.when(d == chip)
        def _():
            tab[T_FROM + b % ALL] = s ^ chip
            tab[T_RANK + b % ALL] = jnp.where(s == chip, row ^ (core * OWN), here)
        return jnp.maximum(most, jnp.where(s == d, 0, total))
    tab[T_MOST] = lax.fori_loop(0, 64, beam, jnp.int32(0))


def make_tables(p1, p2):
    return call(table_kernel, 'tables', GB // 2, GB // 1000, [SMEM] * 2, SMEM, shaped((T_END,), jnp.int32),
                [pltpu.SMEM((BLK,), jnp.int32), pltpu.SMEM((ALL,), jnp.int32)], (p1, p2))


def rms_of(r, g):
    mean_sq = jnp.mean(r * r, axis=-1, keepdims=True)
    return (r * lax.rsqrt(mean_sq + EPS) * g).astype(BF16)


def qkv_kernel(*refs, layer):
    n_res = 3 if layer else 4
    res = refs[:n_res]
    g_ref, cos, sin, wq, wk, wv, out, rout, buf, sem = refs[n_res:]
    core = core_of()

    def copy(w, col, i):
        return pltpu.make_async_copy(w.at[layer, :, pl.ds(pl.multiple_of(col, HEAD), BLK)], buf.at[i], sem.at[i])

    def q_copy(i):
        return copy(wq, (core * OWN + i) * BLK, i)

    def kv_copy(i, w, b):
        return copy(w, (core * 2 + b) * BLK, i)
    kv_blocks = [(OWN + i, (wk, wv)[i // 2], i % 2) for i in range(4)]
    for i in range(OWN):
        q_copy(i).start()
    for block in kv_blocks:
        kv_copy(*block).start()
    if layer:
        r = res[0][...] + (res[1][...] + res[2][...])
    else:
        mine = jnp.concatenate([res[0][...], res[1][...]], axis=0)
        other = jnp.concatenate([res[2][...], res[3][...]], axis=0)
        low = core == 0
        r = jnp.concatenate([jnp.where(low, mine, other), jnp.where(low, other, mine)], axis=0).astype(F32)
    rout[...] = r
    x = rms_of(r, g_ref[layer:layer + 1])
    c = cos[...]
    s = sin[...]

    def rot(v):
        return (v * c + pltpu.roll(v, HEAD // 2, 1) * s).astype(BF16)

    def queries(g, carry):
        for half in range(2):
            q_copy(g * 2 + half).wait()
            y = dot(x, buf[g * 2 + half])
            for j in range(2):
                at = (half * 2 + j) * HEAD
                out[g, :, at:at + HEAD] = rot(y[:, j * HEAD:(j + 1) * HEAD])
        return carry
    lax.fori_loop(0, 4, queries, 0)
    for i, w, b in kv_blocks:
        kv_copy(i, w, b).wait()
        y = dot(x, buf[i])
        for j in range(2):
            part = y[:, j * HEAD:(j + 1) * HEAD]
            if w is wk:
                out[b * 2 + j, :, POS_A:POS_B] = rot(part)
            else:
                out[b * 2 + j, :, POS_B:] = part.astype(BF16)


def run_qkv(layer, res, g, cos, sin, wq, wk, wv):
    dm = wq.shape[1]
    return call(functools.partial(qkv_kernel, layer=layer), f'qkv{layer}', 2 * GB, GB // 40,
                [VMEM] * (len(res) + 3) + [HBM] * 3, [VMEM] * 2,
                [shaped((4, ROWS, 6 * HEAD), BF16), shaped((ROWS, dm), F32)],
                [pltpu.VMEM((12, dm, BLK), BF16), DMA((12,))], (*res, g, cos, sin, wq, wk, wv))


def mlp_kernel(r_ref, g_ref, wg, wu, wd, out, bufg, bufu, bufd, sem, *, layer, steps):
    core = core_of()

    def copies(i):
        slot = lax.rem(i, MLP_SLOTS)
        span = pl.ds(pl.multiple_of((core * steps + i) * BLK, BLK), BLK)
        return (pltpu.make_async_copy(wg.at[layer, :, span], bufg.at[slot], sem.at[0, slot]),
                pltpu.make_async_copy(wu.at[layer, :, span], bufu.at[slot], sem.at[1, slot]),
                pltpu.make_async_copy(wd.at[layer, span], bufd.at[slot], sem.at[2, slot]))
    for i in range(MLP_SLOTS):
        for c in copies(i):
            c.start()
    x = rms_of(r_ref[...], g_ref[layer:layer + 1])
    out[...] = jnp.zeros_like(out)

    def step(i, carry):
        slot = lax.rem(i, MLP_SLOTS)
        for c in copies(i):
            c.wait()
        hid = (jax.nn.silu(dot(x, bufg[slot])) * dot(x, bufu[slot])).astype(BF16)
        out[...] += dot(hid, bufd[slot])

        @pl.when(i + MLP_SLOTS < steps)
        def _():
            for c in copies(i + MLP_SLOTS):
                c.start()
        return carry
    lax.fori_loop(0, steps, step, 0)


def run_mlp(layer, r, g, wg, wu, wd):
    dm, ff = wg.shape[1:]
    return call(functools.partial(mlp_kernel, layer=layer, steps=ff // 2 // BLK), f'mlp{layer}', 12 * GB, GB // 6,
                [VMEM] * 2 + [HBM] * 3, VMEM, shaped(r.shape, F32),
                [pltpu.VMEM((MLP_SLOTS, dm, BLK), BF16), pltpu.VMEM((MLP_SLOTS, dm, BLK), BF16),
                 pltpu.VMEM((MLP_SLOTS, BLK, dm), BF16), DMA((3, MLP_SLOTS))], (r, g, wg, wu, wd))


def vocab_kernel(r_ref, pa, pb, g_ref, w, own, sib, buf, sem):
    core = core_of()
    steps = LOW_VOCAB // BLK - core

    def copy(i):
        slot = lax.rem(i, VOCAB_SLOTS)
        return pltpu.make_async_copy(w.at[:, pl.ds(pl.multiple_of(core * LOW_VOCAB + i * BLK, HEAD), BLK)], buf.at[slot], sem.at[slot])
    for i in range(VOCAB_SLOTS):
        copy(i).start()
    x = rms_of(r_ref[...] + (pa[...] + pb[...]), g_ref[...])
    is_low = core == 0

    def step(i, carry):
        copy(i).wait()
        y = dot(x, buf[lax.rem(i, VOCAB_SLOTS)])
        span = pl.ds(pl.multiple_of(i * BLK, BLK), BLK)
        low, high = y[:ROWS // 2], y[ROWS // 2:]
        own[:, span] = jnp.where(is_low, low, high)
        sib[:, span] = jnp.where(is_low, high, low)

        @pl.when(i + VOCAB_SLOTS < steps)
        def _():
            copy(i + VOCAB_SLOTS).start()
        return carry
    lax.fori_loop(0, steps, step, 0)


def run_vocab(res, g, w):
    half = shaped((ROWS // 2, LOW_VOCAB), F32)
    return call(vocab_kernel, 'vocab', 9 * GB, GB // 8, [VMEM] * 4 + [HBM], [VMEM] * 2, [half, half],
                [pltpu.VMEM((VOCAB_SLOTS, w.shape[0], BLK), BF16), DMA((VOCAB_SLOTS,))], (*res, g, w))


def cand_kernel(own, sib, s1, s2, c1, c2):
    wide = own.shape[1]
    rest = c1.shape[1] - wide
    is_low = core_of() == 0
    for step, (sig, out) in enumerate(((s1, c1), (s2, c2))):
        x = own[step * 8:(step + 1) * 8, :]
        y = sib[step * 8:(step + 1) * 8, :]
        a = jnp.where(is_low, x, y)
        b = jnp.where(is_low, y, x)[:, :rest]
        top = jnp.maximum(jnp.max(a, axis=1, keepdims=True), jnp.max(b, axis=1, keepdims=True))
        total = jnp.sum(jnp.exp(a - top), axis=1, keepdims=True) + jnp.sum(jnp.exp(b - top), axis=1, keepdims=True)
        lse = jnp.log(total)
        sigma = sig[...]
        out[:, :wide] = sigma + ((a - top) - lse)
        out[:, wide:] = sigma + ((b - top) - lse)


def run_cand(own, sib, s1, s2, vocab):
    return call(cand_kernel, 'cand', GB, GB // 100, [VMEM] * 4, [VMEM] * 2, [shaped((8, vocab), F32)] * 2, [], (own, sib, s1, s2))


def heads_kernel(tab, *refs):
    rows, outs, (wide,) = split(refs, 4, 2, 1)
    core = core_of()
    i = pl.program_id(0)
    for half in range(2):
        @pl.when(tab[T_NEED + half * OWN + i] == 1)
        def _(half=half):
            for kind, out in enumerate(outs):
                n = half * 2 + kind
                wide[n] = rows[n][0].reshape(SEQ * KVH, HEAD).astype(F32)
                for c in range(2):
                    @pl.when(core == c)
                    def _(n=n, c=c, out=out):
                        for g in range(GROUPS):
                            out[g, half, 0] = wide[n, pl.ds(c * GROUPS + g, SEQ, stride=KVH), :].astype(BF16)


def run_heads(layer, tab, cache):
    row = pl.BlockSpec((1,) + ROW, lambda i, t: (i, 0, 0, 0))
    block = (GROUPS, 2, 1, SEQ, HEAD)
    kt, vt = pl.pallas_call(
        heads_kernel,
        grid_spec=pltpu.PrefetchScalarGridSpec(
            num_scalar_prefetch=1, grid=(OWN,), in_specs=[row] * 4,
            out_specs=[pl.BlockSpec(block, lambda i, t: (0, 0, i, 0, 0)), pl.BlockSpec(block, lambda i, t: (0, 0, i // 2, 0, i % 2))],
            scratch_shapes=[pltpu.VMEM((4, SEQ * KVH, HEAD), F32)]),
        out_shape=[shaped((GROUPS, 2, OWN, SEQ, HEAD), BF16), shaped((GROUPS, 2, OWN // 2, SEQ, PAIR), BF16)],
        cost_estimate=pl.CostEstimate(flops=2 * GB, bytes_accessed=GB // 80, transcendentals=0),
        compiler_params=pltpu.CompilerParams(vmem_limit_bytes=VLIM), name=f'heads{layer}')(tab, *cache)
    return kt.reshape(GROUPS, ALL * SEQ, HEAD), vt.reshape(GROUPS, OWN, SEQ, PAIR)


def attend(p, allq, kbuf, vbuf, g, row_ref, pick_ref, step_ref):
    n = allq.shape[0]
    full = GROUPS * n
    kv = allq[:, POS_A:]
    onehot = (pick_ref[...] == lax.broadcasted_iota(jnp.int32, (n, n), 1)).astype(BF16)
    kva = dot(onehot, kv)
    kvf = kv.astype(F32)
    stack = lambda x: jnp.concatenate([x] * GROUPS, axis=0)
    q = jnp.concatenate([allq[:, j * HEAD:(j + 1) * HEAD] for j in range(GROUPS)], axis=0)
    qf = q.astype(F32)
    scale = HEAD ** -0.5
    s_a = jnp.sum(qf * stack(kva[:, :HEAD]), axis=1, keepdims=True)
    s_b = jnp.sum(qf * stack(kvf[:, :HEAD]), axis=1, keepdims=True)
    step = stack(step_ref[...])
    rowb = jnp.broadcast_to(stack(row_ref[...]), (full, SEQ))

    def choose(r2, pair, kept):
        kept = jnp.where(rowb == 2 * r2, pair[:, :SEQ], kept)
        return jnp.where(rowb == 2 * r2 + 1, pair[:, SEQ:], kept)
    logits = jnp.zeros((full, SEQ), F32)
    for r2 in range(OWN):
        kk = kbuf[g, r2 * PAIR:(r2 + 1) * PAIR, :]
        s2 = lax.dot_general(q, kk, (((1,), (1,)), ((), ())), preferred_element_type=F32)
        logits = choose(r2, s2, logits)
    col = lax.broadcasted_iota(jnp.int32, (full, SEQ), 1)
    logits = jnp.where(col == p, s_a, jnp.where(col == p + 1, s_b, logits)) * scale
    logits = jnp.where(col <= p + step, logits, -jnp.inf)
    top = jnp.max(logits, axis=1, keepdims=True)
    e = jnp.exp(logits - top)
    pf = (e / jnp.sum(e, axis=1, keepdims=True)).astype(BF16).astype(F32)
    p_a = jnp.sum(jnp.where(col == p, pf, 0.0), axis=1, keepdims=True)
    p_b = jnp.sum(jnp.where(col == p + 1, pf, 0.0), axis=1, keepdims=True)
    old = jnp.where(col < p, pf, 0.0).astype(BF16)
    seen = jnp.zeros((full, HEAD), F32)
    for r2 in range(OWN):
        o2 = dot(old, vbuf[g, r2])
        seen = choose(r2, o2, seen)
    acc = seen + (p_a * stack(kva[:, HEAD:]) + p_b * stack(kvf[:, HEAD:]))
    return jnp.where(rowb >= 0, acc, 0.0).astype(BF16), kva[:ROWS].astype(BF16), kv[:ROWS]


def attn_kernel(pos_ref, row_ref, pick_ref, step_ref, qkv, r_ref, kt, vt, w_out, rout, new,
                kbuf, vbuf, wbuf, qbuf, oown, osend, orecv, psend, precv,
                ksem, vsem, wsem, qs, qr, os, orr, ps, pr, *, layer):
    me = lax.axis_index('beam')
    flip_x = 2 - 4 * ((me // 2) % 2)
    flip_y = 4 - 8 * (me // 4)
    peers = (me + flip_x, me + flip_y, me + flip_x + flip_y)
    mate = me + 1 - 2 * (me % 2)
    core = me % 2

    def k_load(g):
        return pltpu.make_async_copy(kt.at[g], kbuf.at[g], ksem.at[g])

    def v_load(g):
        return pltpu.make_async_copy(vt.at[g], vbuf.at[g], vsem.at[g])

    def w_load(g):
        return pltpu.make_async_copy(w_out.at[layer, pl.ds((core * 4 + g) * KCH, KCH)], wbuf.at[g], wsem.at[g])

    def q_copy(g, m):
        return pltpu.make_async_remote_copy(
            src_ref=qkv.at[g], dst_ref=qbuf.at[g, m], send_sem=qs.at[g, m], recv_sem=qr.at[g, m],
            device_id={'beam': peers[m]}, device_id_type=MESH)

    def o_copy(g, m):
        return pltpu.make_async_remote_copy(
            src_ref=osend.at[g, m], dst_ref=orecv.at[g, m], send_sem=os.at[g, m], recv_sem=orr.at[g, m],
            device_id={'beam': peers[m]}, device_id_type=MESH)

    for g in range(GROUPS):
        k_load(g).start()
        v_load(g).start()
    for g in range(GROUPS):
        w_load(g).start()
    barrier = pltpu.get_barrier_semaphore()
    for peer in peers + (mate,):
        pl.semaphore_signal(barrier, inc=1, device_id={'beam': peer}, device_id_type=MESH)
    pl.semaphore_wait(barrier, 4)
    for g in range(GROUPS):
        for m in range(PEERS):
            q_copy(g, m).start()
    p = pos_ref[0]

    def one_head(g, carry):
        k_load(g).wait()
        v_load(g).wait()
        for m in range(PEERS):
            q_copy(g, m).wait_recv()
        allq = jnp.concatenate([qkv[g]] + [qbuf[g, m] for m in range(PEERS)], axis=0)
        acc, picked, own = attend(p, allq, kbuf, vbuf, g, row_ref, pick_ref, step_ref)
        new[g, :, :PAIR] = picked
        new[g, :, PAIR:] = own
        n = allq.shape[0]
        for m in range(GROUPS):
            for j in range(GROUPS):
                piece = acc[j * n + m * ROWS:j * n + (m + 1) * ROWS]
                if m == 0:
                    oown[g, :, j * HEAD:(j + 1) * HEAD] = piece
                else:
                    osend[g, m - 1, :, j * HEAD:(j + 1) * HEAD] = piece
        for m in range(PEERS):
            o_copy(g, m).start()
        return carry
    lax.fori_loop(0, GROUPS, one_head, 0)

    psend[...] = jnp.zeros_like(psend)

    def project(g, carry):
        w_load(g).wait()
        for m in range(PEERS):
            o_copy(g, m).wait_recv()
        x = (oown[g] + orecv[g, 0]) + (orecv[g, 1] + orecv[g, 2])
        psend[...] += dot(x, wbuf[g])
        return carry
    lax.fori_loop(0, GROUPS, project, 0)

    back = pltpu.make_async_remote_copy(
        src_ref=psend, dst_ref=precv, send_sem=ps, recv_sem=pr, device_id={'beam': mate}, device_id_type=MESH)
    back.start()
    for g in range(GROUPS):
        for m in range(PEERS):
            q_copy(g, m).wait_send()
            o_copy(g, m).wait_send()
    back.wait()
    rout[...] = r_ref[...] + (psend[...] + precv[...])


def run_attn(layer, *args):
    qkv, r, kt, vt, w_out = args[4:]
    vm = pltpu.VMEM
    peer = (GROUPS, PEERS)
    o_parts = vm(peer + (ROWS, KCH), BF16)
    return call(
        functools.partial(attn_kernel, layer=layer), f'attn{layer}', 6 * GB, GB // 50, [SMEM] + [VMEM] * 5 + [HBM] * 3, [VMEM] * 2,
        [shaped(r.shape, F32), shaped((GROUPS, ROWS, POS_A), BF16)],
        [vm(kt.shape, BF16), vm(vt.shape, BF16), vm((GROUPS, KCH, r.shape[1]), BF16), vm(peer + qkv.shape[1:], BF16),
         vm((GROUPS, ROWS, KCH), BF16), o_parts, o_parts, vm(r.shape, F32), vm(r.shape, F32)]
        + [DMA((GROUPS,))] * 3 + [DMA(peer)] * 4 + [DMA] * 2,
        args, collective_id=layer, has_side_effects=True)


def start_chip_row(lr, core, refs, dst, sem):
    for n, ref in enumerate(refs):
        @pl.when(lr // OWN * 2 + core == n)
        def _(ref=ref):
            pltpu.make_async_copy(ref.at[lr % OWN], dst, sem).start()


def pack_kernel(tab, *refs, cap):
    *caches, outs, (buf, rsem, wsem) = split(refs, 4, 4, PEERS, 3)
    core = core_of()

    def each(body):
        for m in range(PEERS):
            for layer in range(2):
                lax.fori_loop(0, cap, lambda i, c, m=m, layer=layer: body(m, layer, i) or c, 0)

    def slot_of(m, layer, i):
        return (m * 2 + layer) * cap + i

    def write(m, layer, i):
        slot = slot_of(m, layer, i)
        return pltpu.make_async_copy(buf.at[slot], outs[m].at[layer * cap + i], wsem.at[slot])

    def begin(m, layer, i):
        slot = slot_of(m, layer, i)
        start_chip_row(tab[m * ALL + i], core, caches[layer], buf.at[slot], rsem.at[slot])

    def onward(m, layer, i):
        slot = slot_of(m, layer, i)
        pltpu.make_async_copy(caches[0][0].at[0], buf.at[slot], rsem.at[slot]).wait()
        write(m, layer, i).start()
    each(begin)
    each(onward)
    each(lambda m, layer, i: write(m, layer, i).wait())


def run_pack(cap, tab, caches):
    slots = 6 * cap
    return call(functools.partial(pack_kernel, cap=cap), f'pack{cap}', GB, slots * GB // 2000, [SMEM] + [HBM] * 8, [HBM] * 3,
                [shaped((2 * cap,) + ROW, BF16)] * 3, [pltpu.VMEM((slots,) + ROW, BF16), DMA((slots,)), DMA((slots,))], (tab, *caches))


def start_pool_row(layer, beam, cap, core, tab, chip_refs, arrived, dst, sem):
    m = tab[T_FROM + beam]
    rank = tab[T_RANK + beam]

    @pl.when(m == 0)
    def _():
        start_chip_row(rank, core, chip_refs, dst, sem)
    for k in range(3):
        @pl.when(m == k + 1)
        def _(k=k):
            pltpu.make_async_copy(arrived[k].at[layer * cap + jnp.minimum(rank, cap - 1)], dst, sem).start()


def back_kernel(tab, *refs, cap):
    *caches, arrived, (out, buf, rsem, wsem) = split(refs, 4, 4, PEERS, 4)
    core = core_of()
    for layer in range(2):
        def begin(i, c, layer=layer):
            start_pool_row(layer, (1 - core) * OWN + i, cap, core, tab, caches[layer], arrived, buf.at[layer * OWN + i], rsem.at[layer * OWN + i])
            return c
        lax.fori_loop(0, OWN, begin, 0)

    def onward(i, c):
        pltpu.make_async_copy(caches[0][0].at[0], buf.at[i], rsem.at[i]).wait()
        pltpu.make_async_copy(buf.at[i], out.at[i], wsem.at[i]).start()
        return c
    lax.fori_loop(0, ALL, onward, 0)

    def end(i, c):
        pltpu.make_async_copy(buf.at[i], out.at[i], wsem.at[i]).wait()
        return c
    lax.fori_loop(0, ALL, end, 0)


def run_back(cap, tab, caches, arrived):
    return call(functools.partial(back_kernel, cap=cap), f'back{cap}', GB, GB // 100, [SMEM] + [HBM] * 11, HBM,
                shaped((ALL,) + ROW, BF16), [pltpu.VMEM((ALL,) + ROW, BF16), DMA((ALL,)), DMA((ALL,))], (tab, *caches, *arrived))


def final_kernel(pos, tab, *refs, cap):
    *caches, arrived, (other,), news, outs, (buf, rsem, wsem) = split(refs, 4, 4, PEERS, 1, 2, 4, 3)
    core = core_of()
    p = pos[0]
    for layer in range(2):
        def begin(i, c, layer=layer):
            mine = layer * ALL + core * OWN + i
            theirs = layer * ALL + (1 - core) * OWN + i
            start_pool_row(layer, core * OWN + i, cap, core, tab, caches[layer], arrived, buf.at[mine], rsem.at[mine])
            pltpu.make_async_copy(other.at[layer * OWN + i], buf.at[theirs], rsem.at[theirs]).start()
            return c
        lax.fori_loop(0, OWN, begin, 0)
    for phase in range(3):
        for layer in range(2):
            for kind in range(2):
                def one(i, c, phase=phase, layer=layer, kind=kind):
                    slot = layer * ALL + kind * OWN + i
                    write = pltpu.make_async_copy(buf.at[slot], outs[layer * 2 + kind].at[i], wsem.at[slot])
                    if phase == 0:
                        pltpu.make_async_copy(other.at[0], buf.at[slot], rsem.at[slot]).wait()
                        buf[slot, pl.ds(p, 1)] = news[layer][i, kind:kind + 1]
                        buf[slot, pl.ds(p + 1, 1)] = news[layer][i, kind + 2:kind + 3]
                    elif phase == 1:
                        write.start()
                    else:
                        write.wait()
                    return c
                lax.fori_loop(0, OWN, one, 0)


def run_final(cap, pos, tab, caches, arrived, other, news):
    return call(functools.partial(final_kernel, cap=cap), f'final{cap}', GB, GB // 60, [SMEM] * 2 + [HBM] * 12 + [VMEM] * 2, [HBM] * 4,
                [shaped((8,) + ROW, BF16)] * 4, [pltpu.VMEM((2 * ALL,) + ROW, BF16), DMA((2 * ALL,)), DMA((2 * ALL,))],
                (pos, tab, *caches, *arrived, other, *news))


def mate(x):
    return swap(x, 1)


tie = lax.optimization_barrier


def send_rows(packed):
    return [swap(x, 2 * (m + 1)) for m, x in enumerate(packed)]


def solution(mesh):
    rows_spec_ = P(('dp', 'beam'))
    full_spec = P()

    def per_device(emb_one, emb_two, parent_one, parent_two, position, scores, k_cache0, v_cache0, k_cache1, v_cache1, w_query, w_key, w_value, w_out, w_gate, w_up, w_down, g_attn, g_mlp, g_final, w_vocab):
        me = lax.axis_index('beam').astype(jnp.int32)
        core = me % 2
        chip = me // 2
        is_low = core == 0
        pos1 = position.astype(jnp.int32)[None]
        g_final = g_final[None]

        def both(own, sib, axis=0):
            return jnp.concatenate([jnp.where(is_low, own, sib), jnp.where(is_low, sib, own)], axis=axis)

        res = (emb_one, emb_two, mate(emb_one), mate(emb_two))
        tab = make_tables(parent_one, parent_two)
        res, k_cache0, v_cache0 = tie((res, k_cache0, v_cache0))
        cache0 = (k_cache0, v_cache0, mate(k_cache0), mate(v_cache0))

        half_dim = HEAD // 2
        inv_freq = ROPE_BASE ** (-2.0 * jnp.arange(half_dim, dtype=F32) / HEAD)
        row_step = (jnp.arange(ROWS, dtype=jnp.int32) // 8) % 2
        angles = (position + row_step).astype(F32)[:, None] * inv_freq[None]
        cosine = jnp.cos(angles)
        sine = jnp.sin(angles)
        cos = jnp.concatenate([cosine, cosine], axis=1)
        sin = jnp.concatenate([-sine, sine], axis=1)

        beams = jnp.arange(4 * ALL, dtype=jnp.int32)
        par1 = parent_one[0]
        par2 = parent_two[0]
        take = lambda values, index: jnp.sum(jnp.where(index[:, None] == beams[None], values[None], 0), axis=1)
        src2 = take(par1, par2)
        pos = jnp.arange(4 * ROWS, dtype=jnp.int32)
        q_step = pos // OWN % 2
        q_beam = (pos // ROWS ^ chip) * ALL + pos // ALL % 2 * OWN + pos % OWN
        q_src = jnp.where(q_step == 0, take(par1, q_beam), take(src2, q_beam))
        q_row = jnp.where(q_src // ALL == chip, q_src % ALL ^ core * OWN, -1)
        par_of = take(par2, q_beam)
        q_pick = jnp.where(q_step == 0, pos, (par_of // ALL ^ chip) * ROWS + par_of // OWN % 2 * ALL + par_of % OWN)
        q_args = [x[:, None] for x in (q_row, q_pick, q_step)]

        pair_scores = both(scores, mate(scores))
        all_scores = jnp.concatenate([pair_scores] + [swap(pair_scores, 2 * m) for m in range(1, 4)])
        score_beam = (beams // ALL ^ chip) * ALL + beams % ALL
        local = me * OWN + jnp.arange(OWN, dtype=jnp.int32)
        sigma = [jnp.sum(jnp.where(take(src, local)[:, None] == score_beam[None], all_scores[None], 0.0), axis=1)[:, None] for src in (par1, src2)]

        news = []
        for layer in range(2):
            qkv, r = run_qkv(layer, res, g_attn, cos, sin, w_query, w_key, w_value)
            if layer == 0:
                qkv, k_cache1, v_cache1 = tie((qkv, k_cache1, v_cache1))
                cache1 = (k_cache1, v_cache1, mate(k_cache1), mate(v_cache1))
                caches = cache0 + cache1
            kt, vt = run_heads(layer, tab, cache1 if layer else cache0)
            r, new = run_attn(layer, pos1, *q_args, qkv, r, kt, vt, w_out)
            if layer == 0:
                r, tab = tie((r, tab))
                received = send_rows(run_pack(CAP, tab, caches))
            else:
                r, arrived = tie((r, received))
                returned = mate(run_back(CAP, tab, caches, arrived))
            new_mate = mate(new)
            part = run_mlp(layer, r, g_mlp, w_gate, w_up, w_down)
            part, new_mate, sigma = tie((part, new_mate, sigma))
            news.append((new, new_mate))
            res = (r, part, mate(part))

        own_logits, mate_logits = run_vocab(res, g_final, w_vocab)
        cand_one, cand_two = run_cand(own_logits, mate(mate_logits), *sigma, w_vocab.shape[1])

        new_rows = []
        for own, other in news:
            pick = lambda x: lax.dynamic_slice(x, (0, core * ALL + OWN, 0), (GROUPS, OWN, KCH)).reshape(GROUPS, OWN, 4, HEAD)
            new_rows.append(jnp.transpose(both(pick(own), pick(other)), (1, 2, 0, 3)))

        def common():
            return tuple(run_final(CAP, pos1, tab, caches, arrived, returned, new_rows))

        def rare():
            full = send_rows(run_pack(ALL, tab, caches))
            return tuple(run_final(ALL, pos1, tab, caches, full, mate(run_back(ALL, tab, caches, full)), new_rows))

        caches_out = lax.cond(tab[T_MOST] > CAP, rare, common)
        return caches_out + (cand_one, cand_two)

    in_specs = (rows_spec_, rows_spec_, P('dp'), P('dp'), full_spec) + (rows_spec_,) * 5 + (full_spec,) * 11
    return jax.shard_map(per_device, mesh=mesh, in_specs=in_specs, out_specs=(rows_spec_,) * 6, check_vma=False)
```
